32 devices in a mesh: region: 2 (over y), super: 16 (over z, x, core).
Axes of the slice: x: 2, y: 2, z: 4, core: 2. Of those that a mesh axis runs over, the one named last changes fastest.
Arguments:
- obs_coords: float32 [2, 131072], P(None, ('region', 'super')), may hold values from 0 to 1, as said below
- obs_values: bfloat16 [64, 131072], P(None, ('region', 'super')), may hold values from -6 to 6
- obs_precision: float32 [131072], P(('region', 'super')), may hold values from 0.0009765625 to 0.009765625
- site_coords: float32 [2, 16384], P(None, ('region', 'super')), may hold values from 0 to 1, as said below
- length_scale: float32 [3], replicated, may hold values from 0.009375 to 0.3, as said below
- global_knots: float32 [2, 256], replicated, may hold values from 0 to 1
- region_knots: float32 [16, 2, 256], P('super'), may hold values from 0 to 1, as said below
- leaf_knots: float32 [32, 2, 256], P(('region', 'super')), may hold values from 0 to 1, as said below
- global_prior: float32 [256, 256], replicated, as said below
- region_prior: float32 [16, 256, 256], P('super'), as said below
- leaf_prior: float32 [32, 256, 256], P(('region', 'super')), as said below
Outputs:
- prediction: float32 [64, 16384], P(None, ('region', 'super'))
The draws below stay inside these ranges and needn't reach their ends.
Inputs may be any that keep to these rules, and one draw needn't show every extreme that they name: `global_prior`: symmetric; each diagonal entry exceeds the sum of magnitudes of the other entries of its row. `region_prior`: each region's matrix symmetric; each diagonal entry exceeds the sum of magnitudes of the other entries of its row. `leaf_prior`: each leaf's matrix symmetric; each diagonal entry exceeds the sum of magnitudes of the other entries of its row. `obs_coords`: the region cells tile the unit square as a grid, each split into a grid of leaf cells; leaf l's observations lie inside leaf l's cell. `site_coords`: leaf l's sites lie inside leaf l's cell. `region_knots`: region g's knots lie inside region g's cell. `leaf_knots`: leaf l's knots lie inside leaf l's cell. `length_scale`: the global scale lies in 0.15 to 0.3, the regional scale in 0.7 to 1.0 times 1 / sqrt(4096), the leaf scale in 0.3 to 0.9 times 1 / sqrt(32).
All inputs are finite; a program needn't handle non-finite values.
Results may differ from the reference program's by a relative error of at most 0.0003.
The reference program's roundings to bfloat16 on the way count: a program that leaves them out, or rounds other values in their place, can miss the bound.
Values sent between devices are 32-bit elements; how exact they have to be, the bound alone decides.
No kernel may reach another device: no remote copies, remote signals or barrier semaphores. Data moves between devices by JAX's collectives and lax.ppermute only.
A program may use at most 64 MiB of HBM per device.

```python
import math
import jax
import jax.numpy as jnp
from jax import lax

R = 256
FIELDS = 64
NOBS = 4096
NSITE = 512
OBS = 131072
N_REGION = 2
N_SUPER = 16


def prior_block(key, count):
    noise = jax.random.normal(key, (count, R, R), jnp.float32) * (0.08 / math.sqrt(R))
    sym = 0.5 * (noise + jnp.swapaxes(noise, 1, 2))
    eye = jnp.eye(R, dtype=jnp.float32)
    offdiag = sym * (1.0 - eye)
    diagonal = 1.25 * jnp.sum(jnp.abs(offdiag), axis=2) + 0.25
    result = offdiag + eye[None, :, :] * diagonal[:, :, None]
    return result


def draw_global_prior(key, part):
    return prior_block(jax.random.fold_in(key, 11), 1)[0]


def draw_region_prior(key, part):
    return prior_block(jax.random.fold_in(key, 12), N_SUPER)


def draw_leaf_prior(key, part):
    return prior_block(jax.random.fold_in(key, 13), N_REGION * N_SUPER)


def grid_shape(count):
    across = 1
    for divisor in range(1, count + 1):
        if count % divisor == 0 and divisor * divisor <= count:
            across = divisor
    return (count // across, across)


def region_cell(region):
    cols_r, rows_r = grid_shape(N_SUPER)
    width = 1.0 / cols_r
    height = 1.0 / rows_r
    left = (region % cols_r).astype(jnp.float32) * width
    bottom = (region // cols_r).astype(jnp.float32) * height
    return (left, bottom, width, height)


def leaf_cell(leaf):
    region = leaf % N_SUPER
    member = leaf // N_SUPER
    left, bottom, width, height = region_cell(region)
    cols_l, rows_l = grid_shape(N_REGION)
    width_l = width / cols_l
    height_l = height / rows_l
    left_l = left + (member % cols_l).astype(jnp.float32) * width_l
    bottom_l = bottom + (member // cols_l).astype(jnp.float32) * height_l
    return (left_l, bottom_l, width_l, height_l)


def place_points(key, leaf):
    left, bottom, width, height = leaf_cell(leaf)
    unit = jax.random.uniform(key, (2,) + leaf.shape, jnp.float32, 0.0, 1.0)
    return jnp.stack([left + unit[0] * width, bottom + unit[1] * height], axis=0)


def draw_obs_coords(key, part):
    leaf = jnp.arange(NOBS * N_REGION * N_SUPER, dtype=jnp.int32) // NOBS
    return place_points(jax.random.fold_in(key, 21), leaf)


def draw_site_coords(key, part):
    leaf = jnp.arange(NSITE * N_REGION * N_SUPER, dtype=jnp.int32) // NSITE
    return place_points(jax.random.fold_in(key, 22), leaf)


def draw_leaf_knots(key, part):
    leaf = jnp.broadcast_to(jnp.arange(N_REGION * N_SUPER, dtype=jnp.int32)[:, None], (N_REGION * N_SUPER, R))
    points = place_points(jax.random.fold_in(key, 23), leaf)
    return jnp.transpose(points, (1, 0, 2))


def draw_region_knots(key, part):
    region = jnp.broadcast_to(jnp.arange(N_SUPER, dtype=jnp.int32)[:, None], (N_SUPER, R))
    left, bottom, width, height = region_cell(region)
    unit = jax.random.uniform(jax.random.fold_in(key, 24), (2, N_SUPER, R), jnp.float32, 0.0, 1.0)
    points = jnp.stack([left + unit[0] * width, bottom + unit[1] * height], axis=0)
    return jnp.transpose(points, (1, 0, 2))


def draw_length_scale(key, part):
    unit = jax.random.uniform(jax.random.fold_in(key, 25), (3,), jnp.float32, 0.0, 1.0)
    spacing = 1.0 / math.sqrt(N_SUPER * R)
    lows = jnp.array([0.15, 0.7 * spacing, 0.3 / math.sqrt(N_REGION * N_SUPER)], jnp.float32)
    highs = jnp.array([0.3, spacing, 0.9 / math.sqrt(N_REGION * N_SUPER)], jnp.float32)
    return jnp.exp(jnp.log(lows) + unit * (jnp.log(highs) - jnp.log(lows)))


def level_of(rng, dims, cuts, least, high):
    def one(axis_at, blocks):
        heights = jax.random.uniform(jax.random.fold_in(jax.random.fold_in(rng, 6), axis_at), (blocks,), jnp.float32, least / len(cuts), high / len(cuts))
        return jnp.repeat(jnp.exp(heights), dims[axis_at] // blocks).reshape((-1,) + (1,) * (len(dims) - axis_at - 1))

    level = one(*cuts[0])
    for cut in cuts[1:]:
        level = level * one(*cut)
    return level


def gaussian(key, shape, deviation, reach, split=(), held_as=jnp.bfloat16):
    factor_of = level_of(key, shape, split, -0.22, 0.18) if split else 1.0
    drawn = jax.random.normal(key, shape, jnp.float32) * deviation * factor_of
    return jnp.minimum(jnp.maximum(drawn, -reach), reach).astype(held_as)


def setup_inputs(seed: int = 0) -> dict:
    splits = jax.random.split(jax.random.key(seed), 12)
    obs_coords = draw_obs_coords(jax.random.fold_in(splits[11], 71), 0)
    obs_values = gaussian(splits[1], (FIELDS, OBS), 1.0, 6.0, ((1, 32),))
    obs_precision = jnp.clip(jnp.exp(math.log(0.009765625) - 2.3025851 * jax.random.uniform(splits[2], (OBS,), jnp.float32) ** level_of(splits[2], (OBS,), ((0, 32),), -0.2, 0.2)), 0.0009765625, 0.009765625)
    site_coords = draw_site_coords(jax.random.fold_in(splits[11], 71), 0)
    length_scale = draw_length_scale(jax.random.fold_in(splits[11], 71), 0)
    global_knots = jnp.clip(jax.random.uniform(splits[5], (2, R), jnp.float32, 0.0, 1.0), 0.0, 1.0)
    region_knots = draw_region_knots(jax.random.fold_in(splits[11], 71), 0)
    leaf_knots = draw_leaf_knots(jax.random.fold_in(splits[11], 71), 0)
    global_prior = draw_global_prior(jax.random.fold_in(splits[11], 71), 0)
    region_prior = draw_region_prior(jax.random.fold_in(splits[11], 71), 0)
    leaf_prior = draw_leaf_prior(jax.random.fold_in(splits[11], 71), 0)
    return dict(obs_coords=obs_coords, obs_values=obs_values, obs_precision=obs_precision, site_coords=site_coords, length_scale=length_scale, global_knots=global_knots, region_knots=region_knots, leaf_knots=leaf_knots, global_prior=global_prior, region_prior=region_prior, leaf_prior=leaf_prior)


HIGH = lax.Precision.HIGHEST

def basis_rows(coords, knots, scale):
    diff_x = coords[0][:, None] - knots[0][None, :]
    diff_y = coords[1][:, None] - knots[1][None, :]
    return jnp.exp(-0.5 * (diff_x * diff_x + diff_y * diff_y) / (scale * scale))

def basis_cols(knots, coords, scale):
    diff_x = knots[0][:, None] - coords[0][None, :]
    diff_y = knots[1][:, None] - coords[1][None, :]
    return jnp.exp(-0.5 * (diff_x * diff_x + diff_y * diff_y) / (scale * scale))

def leaf_terms(coords, values, precision, knots_g, knots_r, knots_l, scales, prior_l):
    weight = jnp.sqrt(precision)[:, None]
    stacked = jnp.concatenate([basis_rows(coords, knots_g, scales[0]), basis_rows(coords, knots_r, scales[1]), basis_rows(coords, knots_l, scales[2]), values.astype(jnp.float32).T], axis=1)
    scaled = (stacked * weight).astype(jnp.bfloat16).astype(jnp.float32)
    gram = jnp.dot(scaled.T, scaled, precision=HIGH)
    cross = gram[2 * R:3 * R, :2 * R]
    factor = jnp.linalg.cholesky(prior_l + gram[2 * R:3 * R, 2 * R:3 * R])
    rhs = jnp.concatenate([cross, gram[2 * R:3 * R, 3 * R:]], axis=1)
    solved = jax.scipy.linalg.cho_solve((factor, True), rhs)
    left = jnp.concatenate([gram[:2 * R, :2 * R], gram[:2 * R, 3 * R:]], axis=1)
    schur = left - jnp.dot(cross.T, solved, precision=HIGH)
    return (schur, solved)

def region_terms(rows, prior_r):
    factor = jnp.linalg.cholesky(prior_r + rows[:, R:2 * R])
    rhs = jnp.concatenate([rows[:, :R], rows[:, 2 * R:]], axis=1)
    solved = jax.scipy.linalg.cho_solve((factor, True), rhs)
    correction = jnp.dot(rows[:, :R].T, solved, precision=HIGH)
    return (solved, correction)

def global_part(schur):
    return jnp.concatenate([schur[:R, :R], schur[:R, 2 * R:]], axis=1)

def reference(obs_coords, obs_values, obs_precision, site_coords, length_scale, global_knots, region_knots, leaf_knots, global_prior, region_prior, leaf_prior):
    coords = obs_coords.reshape(2, N_REGION, N_SUPER, NOBS)
    values = obs_values.reshape(FIELDS, N_REGION, N_SUPER, NOBS)
    precision = obs_precision.reshape(N_REGION, N_SUPER, NOBS)
    sites = site_coords.reshape(2, N_REGION, N_SUPER, NSITE)
    knots_leaf = leaf_knots.reshape(N_REGION, N_SUPER, 2, R)
    prior_leaf = leaf_prior.reshape(N_REGION, N_SUPER, R, R)

    def one_region(index):

        def step(total, member):
            schur, solved = leaf_terms(coords[:, member, index], values[:, member, index], precision[member, index], global_knots, region_knots[index], knots_leaf[member, index], length_scale, prior_leaf[member, index])
            return (total + schur, solved)
        start = jnp.zeros((2 * R, 2 * R + FIELDS), jnp.float32)
        total, solved = lax.scan(step, start, jnp.arange(N_REGION))
        region_solved, correction = region_terms(total[R:2 * R], region_prior[index])
        return (global_part(total) - correction, region_solved, solved)
    pieces, region_solved, leaf_solved = lax.map(one_region, jnp.arange(N_SUPER))
    upper = lax.optimization_barrier(jnp.sum(pieces, axis=0))
    factor = jnp.linalg.cholesky(global_prior + upper[:, :R])
    global_weights = jax.scipy.linalg.cho_solve((factor, True), upper[:, R:])

    def predict_region(index):
        solved_r = region_solved[index]
        region_weights = solved_r[:, R:] - jnp.dot(solved_r[:, :R], global_weights, precision=HIGH)
        upper_weights = jnp.concatenate([global_weights, region_weights], axis=0)

        def predict_leaf(member):
            solved_l = leaf_solved[index, member]
            leaf_weights = solved_l[:, 2 * R:] - jnp.dot(solved_l[:, :2 * R], upper_weights, precision=HIGH)
            weights = jnp.concatenate([upper_weights, leaf_weights], axis=0)
            place = sites[:, member, index]
            table = jnp.concatenate([basis_cols(global_knots, place, length_scale[0]), basis_cols(region_knots[index], place, length_scale[1]), basis_cols(knots_leaf[member, index], place, length_scale[2])], axis=0)
            return jnp.dot(weights.T, table, precision=HIGH)
        return lax.map(predict_leaf, jnp.arange(N_REGION))
    blocks = lax.map(predict_region, jnp.arange(N_SUPER))
    return jnp.transpose(blocks, (2, 1, 0, 3)).reshape(FIELDS, N_REGION * N_SUPER * NSITE)
```

```python
import functools

import jax
import jax.numpy as jnp
from jax import lax
from jax.experimental import pallas as pl
from jax.experimental.pallas import tpu as pltpu
from jax.sharding import PartitionSpec as P

HIGH = lax.Precision.HIGHEST
F32 = jnp.float32


def mm(a, b, ca=1, cb=0):
    return lax.dot_general(a, b, (((ca,), (cb,)), ((), ())), precision=HIGH, preferred_element_type=F32)


def spd_inverse(a):
    n = a.shape[0]
    groups = n // 8
    rows = [a[8 * i : 8 * i + 8, :] for i in range(groups)]
    lane = lax.broadcasted_iota(jnp.int32, (8, n), 1)
    sub = lax.broadcasted_iota(jnp.int32, (8, n), 0)
    for g in range(groups):

        def col(x, k, g=g):
            return jnp.broadcast_to(x[:, 8 * g + k : 8 * g + k + 1], (8, n))

        p = rows[g]
        c = [col(p, k) for k in range(8)]
        inside = (lane >= 8 * g) & (lane < 8 * g + 8)
        p = jnp.where(inside, jnp.where(lane - 8 * g == sub, 1.0, 0.0), p)
        for k in range(8):
            here = sub == k
            r = 1.0 / jnp.broadcast_to(c[k][k : k + 1, :], (8, n))
            for m in range(k + 1, 8):
                s = jnp.broadcast_to(c[m][k : k + 1, :], (8, n)) * r
                c[m] = jnp.where(here, s, c[m] - c[k] * s)
            s = jnp.broadcast_to(p[k : k + 1, :], (8, n)) * r
            p = jnp.where(here, s, p - c[k] * s)
        pr = [jnp.broadcast_to(p[k : k + 1, :], (8, n)) for k in range(8)]
        for i in range(groups):
            if i == g:
                continue
            old = rows[i]
            t = [col(old, k) * pr[k] for k in range(8)]
            while len(t) > 1:
                t = [t[q] + t[q + 1] for q in range(0, len(t), 2)]
            rows[i] = jnp.where(inside, 0.0, old) - t[0]
        rows[g] = p
    return jnp.concatenate(rows, axis=0)


def spd_solve(a, b):
    h = a.shape[0] // 2
    a12 = a[:h, h:]
    i1 = spd_inverse(a[:h, :h])
    t = mm(i1, a12)
    i2 = spd_inverse(a[h:, h:] - mm(a12, t, 0, 0))
    x2 = mm(i2, b[h:] - mm(t, b[:h], 0, 0))
    x1 = mm(i1, b[:h]) - mm(t, x2)
    return jnp.concatenate([x1, x2], axis=0)


def leaf_kernel(chunks, scale_ref, knots_ref, coords_ref, values_ref, prec_ref, prior_ref,
                rows_ref, upper_ref, solved_ref, za, zb, acc_g, acc_r, acc_v):
    r = prior_ref.shape[0]
    width = za.shape[1]

    def fill(z, chunk):
        cols = pl.ds(pl.multiple_of(chunk * width, width), width)
        px = coords_ref[0:1, cols]
        py = coords_ref[1:2, cols]
        weight = jnp.sqrt(prec_ref[0:1, cols])
        for level in range(3):
            factor = -0.5 / (scale_ref[level] * scale_ref[level])
            dx = knots_ref[level * r : (level + 1) * r, 0:1] - px
            dy = knots_ref[level * r : (level + 1) * r, 1:2] - py
            basis = jnp.exp((dx * dx + dy * dy) * factor)
            z[level * r : (level + 1) * r, :] = (basis * weight).astype(jnp.bfloat16)
        z[3 * r :, :] = (values_ref[:, cols].astype(F32) * weight).astype(jnp.bfloat16)

    def gram(z):
        for level, acc in enumerate((acc_g, acc_r, acc_v)):
            acc[...] += lax.dot_general(
                z[level * r :, :], z[level * r : (level + 1) * r, :], (((1,), (1,)), ((), ())),
                preferred_element_type=F32,
            )

    acc_g[...] = jnp.zeros_like(acc_g)
    acc_r[...] = jnp.zeros_like(acc_r)
    acc_v[...] = jnp.zeros_like(acc_v)
    fill(za, 0)

    def step(i, carry):
        fill(zb, 2 * i + 1)
        gram(za)
        fill(za, jnp.minimum(2 * i + 2, chunks - 1))
        gram(zb)
        return carry

    lax.fori_loop(0, chunks // 2, step, 0)
    y_cols = jnp.transpose(jnp.concatenate([acc_g[3 * r :, :], acc_r[2 * r :, :], acc_v[r:, :]], axis=1))
    cross_g = acc_g[2 * r : 3 * r, :]
    cross_r = acc_r[r : 2 * r, :]
    x = spd_solve(prior_ref[...] + acc_v[:r, :], jnp.concatenate([cross_g, cross_r, y_cols[2 * r :]], axis=1))
    solved_ref[...] = x
    left = jnp.concatenate([acc_g[r : 2 * r, :], acc_r[:r, :], y_cols[r : 2 * r]], axis=1)
    rows_ref[...] = left - mm(cross_r, x, 0, 0)
    left = jnp.concatenate([acc_g[:r, :], y_cols[:r]], axis=1)
    upper_ref[...] = left - mm(cross_g, jnp.concatenate([x[:, :r], x[:, 2 * r :]], axis=1), 0, 0)


def region_kernel(share, half_ref, own_ref, other_ref, prior_ref, upper_ref, solved_ref, keep_ref, send_ref, delta):
    r = prior_ref.shape[0]
    rows = own_ref[...] + other_ref[...]
    cross = rows[:, :r]
    x = spd_solve(prior_ref[...] + rows[:, r : 2 * r], jnp.concatenate([cross, rows[:, 2 * r :]], axis=1))
    solved_ref[...] = x
    delta[...] = upper_ref[...] - mm(cross, x, 0, 0) * share
    h = r // 2
    mine = half_ref[0] * h
    keep_ref[...] = delta[pl.ds(pl.multiple_of(mine, h), h), :]
    send_ref[...] = delta[pl.ds(pl.multiple_of(h - mine, h), h), :]


def global_kernel(half_ref, mine_ref, other_ref, prior_ref, region_ref, leaf_ref, table_ref, out_ref, upper):
    r = prior_ref.shape[0]
    h = r // 2
    mine = half_ref[0] * h
    upper[pl.ds(pl.multiple_of(mine, h), h), :] = mine_ref[...]
    upper[pl.ds(pl.multiple_of(h - mine, h), h), :] = other_ref[...]
    w_g = spd_solve(prior_ref[...] + upper[:, :r], upper[:, r:])
    w_r = region_ref[:, r:] - mm(region_ref[:, :r], w_g)
    w_l = leaf_ref[:, 2 * r :] - mm(leaf_ref[:, : 2 * r], jnp.concatenate([w_g, w_r], axis=0))
    out_ref[...] = mm(jnp.concatenate([w_g, w_r, w_l], axis=0), table_ref[...], 0, 0)


def basis_cols(knots, coords, scale):
    diff_x = knots[0][:, None] - coords[0][None, :]
    diff_y = knots[1][:, None] - coords[1][None, :]
    return jnp.exp(-0.5 * (diff_x * diff_x + diff_y * diff_y) / (scale * scale))


SMEM = pl.BlockSpec(memory_space=pltpu.SMEM)
VMEM = pl.BlockSpec(memory_space=pltpu.VMEM)


def shape(*dims):
    return jax.ShapeDtypeStruct(dims, F32)


def swap_sum(x, axis, size, first=0):
    step = 1 << first
    while step < size:
        x = x + lax.ppermute(x, axis, [(i, i ^ step) for i in range(size)])
        step *= 2
    return x


def shards(n_region, n_super, obs_coords, obs_values, obs_precision, site_coords, length_scale,
           global_knots, region_knots, leaf_knots, global_prior, region_prior, leaf_prior):
    r = global_knots.shape[1]
    fields, nobs = obs_values.shape
    knots = jnp.concatenate([global_knots, region_knots[0], leaf_knots[0]], axis=1).T
    width = 512
    chunks = nobs // width
    rows, upper, solved = pl.pallas_call(
        functools.partial(leaf_kernel, chunks),
        out_shape=(shape(r, 2 * r + fields), shape(r, r + fields), shape(r, 2 * r + fields)),
        in_specs=[SMEM] + [VMEM] * 5,
        out_specs=(VMEM,) * 3,
        scratch_shapes=[
            pltpu.VMEM((3 * r + fields, width), jnp.bfloat16),
            pltpu.VMEM((3 * r + fields, width), jnp.bfloat16),
            pltpu.VMEM((3 * r + fields, r), F32),
            pltpu.VMEM((2 * r + fields, r), F32),
            pltpu.VMEM((r + fields, r), F32),
        ],
        name="leaf",
    )(length_scale, knots, obs_coords, obs_values, obs_precision[None, :], leaf_prior[0])
    half = (lax.axis_index("super") & 1).astype(jnp.int32)[None]
    pair = [(i, i ^ 1) for i in range(n_super)]
    own = rows
    step = 1
    other = lax.ppermute(own, "region", [(i, i ^ step) for i in range(n_region)])
    while step * 2 < n_region:
        own = own + other
        step *= 2
        other = lax.ppermute(own, "region", [(i, i ^ step) for i in range(n_region)])
    h = r // 2
    region_solved, keep, send = pl.pallas_call(
        functools.partial(region_kernel, 1.0 / n_region),
        out_shape=(shape(r, r + fields), shape(h, r + fields), shape(h, r + fields)),
        in_specs=[SMEM] + [VMEM] * 4,
        out_specs=(VMEM,) * 3,
        scratch_shapes=[pltpu.VMEM((r, r + fields), F32)],
        name="region",
    )(half, own, other, region_prior[0], upper)
    mine = keep + lax.ppermute(send, "super", pair)
    mine = swap_sum(mine, "region", n_region)
    mine = swap_sum(mine, "super", n_super, first=1)
    other = lax.ppermute(mine, "super", pair)
    table = jnp.concatenate(
        [
            basis_cols(global_knots, site_coords, length_scale[0]),
            basis_cols(region_knots[0], site_coords, length_scale[1]),
            basis_cols(leaf_knots[0], site_coords, length_scale[2]),
        ],
        axis=0,
    )
    return pl.pallas_call(
        global_kernel,
        out_shape=shape(fields, site_coords.shape[1]),
        in_specs=[SMEM] + [VMEM] * 6,
        out_specs=VMEM,
        scratch_shapes=[pltpu.VMEM((r, r + fields), F32)],
        name="predict",
    )(half, mine, other, global_prior, region_solved, solved, table)


def solution(mesh):
    in_specs = (
        P(None, ("region", "super")),
        P(None, ("region", "super")),
        P(("region", "super")),
        P(None, ("region", "super")),
        P(),
        P(),
        P("super", None, None),
        P(("region", "super"), None, None),
        P(),
        P("super", None, None),
        P(("region", "super"), None, None),
    )
    out_specs = P(None, ("region", "super"))
    body = functools.partial(shards, mesh.shape["region"], mesh.shape["super"])
    return jax.shard_map(body, mesh=mesh, in_specs=in_specs, out_specs=out_specs, check_vma=False)
```

```python
import functools

import jax
import jax.numpy as jnp
from jax import lax
from jax.experimental import pallas as pl
from jax.experimental.pallas import tpu as pltpu
from jax.sharding import PartitionSpec as P


HIGH = lax.Precision.HIGHEST
F32 = jnp.float32


def mm(a, b, ca=1, cb=0):
    return lax.dot_general(a, b, (((ca,), (cb,)), ((), ())), precision=HIGH, preferred_element_type=F32)


def spd_inverse(a):
    n = a.shape[0]
    groups = n // 8
    rows = [a[8 * i : 8 * i + 8, :] for i in range(groups)]
    lane = lax.broadcasted_iota(jnp.int32, (8, n), 1)
    sub = lax.broadcasted_iota(jnp.int32, (8, n), 0)
    for g in range(groups):

        def col(x, k, g=g):
            return jnp.broadcast_to(x[:, 8 * g + k : 8 * g + k + 1], (8, n))

        p = rows[g]
        c = [col(p, k) for k in range(8)]
        inside = (lane >= 8 * g) & (lane < 8 * g + 8)
        p = jnp.where(inside, jnp.where(lane - 8 * g == sub, 1.0, 0.0), p)
        for k in range(8):
            here = sub == k
            r = 1.0 / jnp.broadcast_to(c[k][k : k + 1, :], (8, n))
            for m in range(k + 1, 8):
                s = jnp.broadcast_to(c[m][k : k + 1, :], (8, n)) * r
                c[m] = jnp.where(here, s, c[m] - c[k] * s)
            s = jnp.broadcast_to(p[k : k + 1, :], (8, n)) * r
            p = jnp.where(here, s, p - c[k] * s)
        pr = [jnp.broadcast_to(p[k : k + 1, :], (8, n)) for k in range(8)]
        for i in range(groups):
            if i == g:
                continue
            old = rows[i]
            t = [col(old, k) * pr[k] for k in range(8)]
            while len(t) > 1:
                t = [t[q] + t[q + 1] for q in range(0, len(t), 2)]
            rows[i] = jnp.where(inside, 0.0, old) - t[0]
        rows[g] = p
    return jnp.concatenate(rows, axis=0)


def spd_factor(a):
    h = a.shape[0] // 2
    a12 = a[:h, h:]
    i1 = spd_inverse(a[:h, :h])
    t = mm(i1, a12)
    i2 = spd_inverse(a[h:, h:] - mm(a12, t, 0, 0))
    return i1, t, i2


def spd_apply(factor, b):
    i1, t, i2 = factor
    h = t.shape[0]
    x2 = mm(i2, b[h:] - mm(t, b[:h], 0, 0))
    x1 = mm(i1, b[:h]) - mm(t, x2)
    return jnp.concatenate([x1, x2], axis=0)


def pack_halves(f):
    h = f.shape[0] // 2
    q = h // 2
    first = jnp.concatenate([f[:h, :h], f[:h, h : h + q], f[:h, 2 * h :]], axis=1)
    second = jnp.concatenate([f[h:, h : 2 * h], f[:h, h + q : 2 * h], f[h:, 2 * h :]], axis=1)
    return first, second


def knot_columns(refs):
    rows = [refs[0][...], refs[1][0], refs[2][0]]
    rows.append(jnp.zeros_like(rows[0]))
    return jnp.transpose(jnp.concatenate(rows, axis=0))


def basis(knots, level, px, py, scale):
    dx = knots[:, 2 * level : 2 * level + 1] - px
    dy = knots[:, 2 * level + 1 : 2 * level + 2] - py
    return jnp.exp((dx * dx + dy * dy) * (-0.5 / (scale * scale)))


def leaf_kernel(chunks, scale_ref, kg_ref, kr_ref, kl_ref, coords_ref, values_ref, prec_ref, prior_ref,
                pair_ref, factor_ref, acc_g, acc_r, acc_v, za, zb, knots_ref):
    r = prior_ref.shape[1]
    h = r // 2
    width = za.shape[1]
    knots_ref[...] = knot_columns((kg_ref, kr_ref, kl_ref))

    def fill(z, chunk):
        cols = pl.ds(pl.multiple_of(chunk * width, width), width)
        px = coords_ref[0:1, cols]
        py = coords_ref[1:2, cols]
        weight = jnp.sqrt(prec_ref[0:1, cols])
        knots = knots_ref[...]
        for level in range(3):
            table = basis(knots, level, px, py, scale_ref[level])
            z[level * r : (level + 1) * r, :] = (table * weight).astype(jnp.bfloat16)
        z[3 * r :, :] = (values_ref[:, cols].astype(F32) * weight).astype(jnp.bfloat16)

    def gram(z):
        for level, acc in enumerate((acc_g, acc_r, acc_v)):
            acc[...] += lax.dot_general(
                z[level * r :, :], z[level * r : (level + 1) * r, :], (((1,), (1,)), ((), ())),
                preferred_element_type=F32,
            )

    acc_g[...] = jnp.zeros_like(acc_g)
    acc_r[...] = jnp.zeros_like(acc_r)
    acc_v[...] = jnp.zeros_like(acc_v)
    fill(za, 0)

    def step(i, carry):
        fill(zb, 2 * i + 1)
        gram(za)
        fill(za, jnp.minimum(2 * i + 2, chunks - 1))
        gram(zb)
        return carry

    lax.fori_loop(0, chunks // 2, step, 0)
    cross = acc_r[r : 2 * r, :]
    factor = spd_factor(prior_ref[0] + acc_v[:r, :])
    for i in range(3):
        factor_ref[i] = factor[i]
    s = acc_r[:r, :] - mm(cross, spd_apply(factor, cross), 0, 0)
    pair_ref[...] = jnp.concatenate([s[:h, :h], s[:h, h:], s[h:, h:]], axis=1)


def leaf_rest_kernel(half_ref, scale_ref, kg_ref, kr_ref, kl_ref, sites_ref, factor_ref, acc_g, acc_r, acc_v,
                     solved_ref, cross_ref, keep_ref, send_ref, table_ref, pieces):
    r = acc_g.shape[1]
    h = r // 2
    y_cols = jnp.transpose(jnp.concatenate([acc_g[3 * r :, :], acc_r[2 * r :, :], acc_v[r:, :]], axis=1))
    cross_g = acc_g[2 * r : 3 * r, :]
    cross_r = acc_r[r : 2 * r, :]
    factor = (factor_ref[0], factor_ref[1], factor_ref[2])
    x = spd_apply(factor, jnp.concatenate([cross_g, cross_r, y_cols[2 * r :]], axis=1))
    solved_ref[...] = x
    x = jnp.concatenate([x[:, :r], x[:, 2 * r :]], axis=1)
    rows = jnp.concatenate([acc_g[r : 2 * r, :], y_cols[r : 2 * r]], axis=1) - mm(cross_r, x, 0, 0)
    cross_ref[...] = jnp.concatenate([rows[:h, :r], rows[h:, :r], rows[:h, r:], rows[h:, r:]], axis=1)
    upper = jnp.concatenate([acc_g[:r, :], y_cols[:r]], axis=1) - mm(cross_g, x, 0, 0)
    pieces[0], pieces[1] = pack_halves(upper)
    keep_ref[...] = pieces[half_ref[0]]
    send_ref[...] = pieces[1 - half_ref[0]]
    knots = knot_columns((kg_ref, kr_ref, kl_ref))
    for level in range(3):
        table_ref[level * r : (level + 1) * r, :] = basis(
            knots, level, sites_ref[0:1, :], sites_ref[1:2, :], scale_ref[level]
        )


def region_factor_kernel(own_ref, other_ref, prior_ref, after_ref, factor_ref):
    h = own_ref.shape[0]
    s = own_ref[...] + other_ref[...]
    lower = jnp.concatenate([s[:, h : 2 * h], s[:, 2 * h :]], axis=0)
    upper = jnp.concatenate([s[:, :h], jnp.zeros_like(s[:, :h])], axis=0)
    factor = spd_factor(prior_ref[0] + jnp.concatenate([upper, lower], axis=1))
    for i in range(3):
        factor_ref[i] = factor[i]


def region_kernel(half_ref, factor_ref, own_ref, other_ref, upper_ref, solved_ref, keep_ref, send_ref, pieces):
    h = own_ref.shape[0]
    r = 2 * h
    rows = own_ref[...] + other_ref[...]
    fields = (rows.shape[1] - 2 * r) // 2
    cross = jnp.concatenate([rows[:, :r], rows[:, r : 2 * r]], axis=0)
    y = jnp.concatenate([rows[:, 2 * r : 2 * r + fields], rows[:, 2 * r + fields :]], axis=0)
    x = spd_apply((factor_ref[0], factor_ref[1], factor_ref[2]), jnp.concatenate([cross, y], axis=1))
    solved_ref[...] = x
    pieces[0], pieces[1] = pack_halves(-mm(cross, x, 0, 0))
    keep_ref[...] = upper_ref[...] + pieces[half_ref[0]]
    send_ref[...] = pieces[1 - half_ref[0]]


def global_kernel(half_ref, mine_ref, other_ref, prior_ref, region_ref, leaf_ref, table_ref, out_ref, pieces):
    r = prior_ref.shape[0]
    h = r // 2
    q = h // 2
    pieces[half_ref[0]] = mine_ref[...]
    pieces[1 - half_ref[0]] = other_ref[...]
    a = pieces[0]
    b = pieces[1]
    top = jnp.concatenate([a[:, : h + q], b[:, h : h + q]], axis=1)
    low = jnp.concatenate([jnp.zeros_like(b[:, :h]), b[:, :h]], axis=1)
    y = jnp.concatenate([a[:, h + q :], b[:, h + q :]], axis=0)
    w_g = spd_apply(spd_factor(prior_ref[...] + jnp.concatenate([top, low], axis=0)), y)
    w_r = region_ref[:, r:] - mm(region_ref[:, :r], w_g)
    w_l = leaf_ref[:, 2 * r :] - mm(leaf_ref[:, : 2 * r], jnp.concatenate([w_g, w_r], axis=0))
    out_ref[...] = mm(jnp.concatenate([w_g, w_r, w_l], axis=0), table_ref[...], 0, 0)


SMEM = pl.BlockSpec(memory_space=pltpu.SMEM)
VMEM = pl.BlockSpec(memory_space=pltpu.VMEM)
ANY = pl.BlockSpec(memory_space=pl.ANY)


def in_vmem(x):
    return pltpu.with_memory_space_constraint(x, pltpu.VMEM)


def shape(*dims):
    return jax.ShapeDtypeStruct(dims, F32)


def cost(flops, transcendentals):
    return pl.CostEstimate(flops=6 * flops, transcendentals=transcendentals, bytes_accessed=1 << 21)


def swap(x, axis, size, mask):
    return lax.ppermute(x, axis, [(i, i ^ mask) for i in range(size)])


def masks(size, first):
    bits = [b for b in range(first, size.bit_length() - 1)]
    return [(3 << (b - 1)) if b >= 3 else (1 << b) for b in bits]


def swap_halfway(x, axis, size):
    steps = masks(size, 0)
    for mask in steps[:-1]:
        x = x + swap(x, axis, size, mask)
    return x, swap(x, axis, size, steps[-1])


def shards(n_region, n_super, obs_coords, obs_values, obs_precision, site_coords, length_scale,
           global_knots, region_knots, leaf_knots, global_prior, region_prior, leaf_prior):
    r = global_knots.shape[1]
    h = r // 2
    fields, nobs = obs_values.shape
    nsite = site_coords.shape[1]
    width = 512
    knots = (global_knots, region_knots, leaf_knots)
    half = (lax.axis_index("super") & 1).astype(jnp.int32)[None]
    tall = [shape((3 - level) * r + fields, r) for level in range(3)]
    z = pltpu.VMEM((3 * r + fields, width), jnp.bfloat16)
    own, factor, acc_g, acc_r, acc_v = pl.pallas_call(
        functools.partial(leaf_kernel, nobs // width),
        out_shape=(shape(h, 3 * h), shape(3, h, h), *tall),
        in_specs=[SMEM] + [VMEM] * 7,
        out_specs=(VMEM,) * 5,
        scratch_shapes=[z, z, pltpu.VMEM((r, 8), F32)],
        name="leaf",
        cost_estimate=cost(2 * nobs * (3 * r + fields) ** 2, 3 * r * nobs),
    )(length_scale, *knots, obs_coords, obs_values, obs_precision[None, :], leaf_prior)
    own, other = swap_halfway(own, "region", n_region)
    pieces = pltpu.VMEM((2, h, r), F32)
    solved, cross, keep, send, table = pl.pallas_call(
        leaf_rest_kernel,
        out_shape=(shape(r, 2 * r + fields), shape(h, 2 * r + 2 * fields), shape(h, r), shape(h, r), shape(3 * r, nsite)),
        in_specs=[SMEM] * 2 + [VMEM] * 8,
        out_specs=(VMEM,) * 5,
        scratch_shapes=[pieces],
        name="leaf_rest",
        cost_estimate=cost(r * r * (8 * r + 6 * fields), 3 * r * nsite),
    )(half, length_scale, *knots, site_coords, factor, acc_g, acc_r, acc_v)
    region_factor = pl.pallas_call(
        region_factor_kernel,
        out_shape=shape(3, h, h),
        in_specs=[VMEM] * 3 + [ANY],
        out_specs=VMEM,
        name="region_factor",
        cost_estimate=cost(8 * r * r * r, r),
    )(own, in_vmem(other), region_prior, table)
    own, other = swap_halfway(cross, "region", n_region)
    upper = keep + swap(send, "super", n_super, 1)
    for mask in masks(n_region, 0):
        upper = upper + swap(upper, "region", n_region, mask)
    region_solved, keep, send = pl.pallas_call(
        region_kernel,
        out_shape=(shape(r, r + fields), shape(h, r), shape(h, r)),
        in_specs=[SMEM] + [VMEM] * 4,
        out_specs=(VMEM,) * 3,
        scratch_shapes=[pieces],
        name="region",
        cost_estimate=cost(4 * r * r * (r + fields), r),
    )(half, region_factor, own, in_vmem(other), in_vmem(upper))
    mine = keep + swap(send, "super", n_super, 1)
    for mask in masks(n_super, 1):
        mine = mine + swap(mine, "super", n_super, mask)
    other = swap(mine, "super", n_super, 1)
    return pl.pallas_call(
        global_kernel,
        out_shape=shape(fields, nsite),
        in_specs=[SMEM] + [VMEM] * 6,
        out_specs=VMEM,
        scratch_shapes=[pieces],
        name="predict",
        cost_estimate=cost(8 * r * r * r, r),
    )(half, in_vmem(mine), in_vmem(other), global_prior, region_solved, solved, table)


def solution(mesh):
    in_specs = (
        P(None, ("region", "super")),
        P(None, ("region", "super")),
        P(("region", "super")),
        P(None, ("region", "super")),
        P(),
        P(),
        P("super", None, None),
        P(("region", "super"), None, None),
        P(),
        P("super", None, None),
        P(("region", "super"), None, None),
    )
    out_specs = P(None, ("region", "super"))
    body = functools.partial(shards, mesh.shape["region"], mesh.shape["super"])

    return jax.shard_map(body, mesh=mesh, in_specs=in_specs, out_specs=out_specs, check_vma=False)
```

```python
import functools

import jax
import jax.numpy as jnp
from jax import lax
from jax.experimental import pallas as pl
from jax.experimental.pallas import tpu as pltpu
from jax.sharding import PartitionSpec as P


HIGH = lax.Precision.HIGHEST
F32 = jnp.float32


def mm(a, b, ca=1, cb=0):
    return lax.dot_general(a, b, (((ca,), (cb,)), ((), ())), precision=HIGH, preferred_element_type=F32)


def spd_inverse(a):
    n = a.shape[0]
    groups = n // 8
    rows = [a[8 * i : 8 * i + 8, :] for i in range(groups)]
    lane = lax.broadcasted_iota(jnp.int32, (8, n), 1)
    sub = lax.broadcasted_iota(jnp.int32, (8, n), 0)

    def col(x, j):
        return jnp.broadcast_to(x[:, j : j + 1], (8, n))

    def row(x, k):
        return jnp.take_along_axis(x, jnp.full((8, n), k, jnp.int32), axis=0, mode="promise_in_bounds")

    for g in range(groups):
        p = rows[g]
        c = [col(p, 8 * g + k) for k in range(8)]
        b = {i: [] for i in range(groups) if i != g}
        for k in range(8):
            for i in b:
                b[i].append(col(rows[i], 8 * g + k))
        inside = (lane >= 8 * g) & (lane < 8 * g + 8)
        p = jnp.where(inside, jnp.where(lane - 8 * g == sub, 1.0, 0.0), p)
        pivot = row(c[0], 0)
        for k in range(8):
            here = sub == k
            r = 1.0 / pivot
            for m in range(k + 1, 8):
                s = row(c[m], k) * r
                left = c[m] - c[k] * s
                if m == k + 1:
                    pivot = row(left, m)
                c[m] = jnp.where(here, s, left)
            s = row(p, k) * r
            p = jnp.where(here, s, p - c[k] * s)
        pr = [row(p, k) for k in range(8)]
        for i in b:
            t = [b[i][k] * pr[k] for k in range(8)]
            while len(t) > 1:
                t = [t[q] + t[q + 1] for q in range(0, len(t), 2)]
            rows[i] = jnp.where(inside, 0.0, rows[i]) - t[0]
        rows[g] = p
    return jnp.concatenate(rows, axis=0)


def spd_factor(a):
    h = a.shape[0] // 2
    a12 = a[:h, h:]
    i1 = spd_inverse(a[:h, :h])
    t = mm(i1, a12)
    i2 = spd_inverse(a[h:, h:] - mm(a12, t, 0, 0))
    return i1, t, i2


def spd_apply(factor, b):
    i1, t, i2 = factor
    h = t.shape[0]
    x2 = mm(i2, b[h:] - mm(t, b[:h], 0, 0))
    x1 = mm(i1, b[:h]) - mm(t, x2)
    return jnp.concatenate([x1, x2], axis=0)


def pack_halves(f):
    h = f.shape[0] // 2
    q = h // 2
    first = jnp.concatenate([f[:h, :h], f[:h, h : h + q], f[:h, 2 * h :]], axis=1)
    second = jnp.concatenate([f[h:, h : 2 * h], f[:h, h + q : 2 * h], f[h:, 2 * h :]], axis=1)
    return first, second


def knot_columns(refs):
    rows = [refs[0][...], refs[1][0], refs[2][0]]
    rows.append(jnp.zeros_like(rows[0]))
    return jnp.transpose(jnp.concatenate(rows, axis=0))


def basis(knots, level, px, py, scale):
    dx = knots[:, 2 * level : 2 * level + 1] - px
    dy = knots[:, 2 * level + 1 : 2 * level + 2] - py
    return jnp.exp((dx * dx + dy * dy) * (-0.5 / (scale * scale)))


def leaf_kernel(chunks, scale_ref, kg_ref, kr_ref, kl_ref, coords_ref, values_ref, prec_ref, prior_ref,
                pair_ref, factor_ref, acc_g, acc_r, acc_v, za, zb, knots_ref):
    r = prior_ref.shape[1]
    h = r // 2
    width = za.shape[1]
    knots_ref[...] = knot_columns((kg_ref, kr_ref, kl_ref))

    def fill(z, chunk):
        cols = pl.ds(pl.multiple_of(chunk * width, width), width)
        px = coords_ref[0:1, cols]
        py = coords_ref[1:2, cols]
        weight = jnp.sqrt(prec_ref[0:1, cols])
        knots = knots_ref[...]
        for level in range(3):
            table = basis(knots, level, px, py, scale_ref[level])
            z[level * r : (level + 1) * r, :] = (table * weight).astype(jnp.bfloat16)
        z[3 * r :, :] = (values_ref[:, cols].astype(F32) * weight).astype(jnp.bfloat16)

    def gram(z):
        for level, acc in enumerate((acc_g, acc_r, acc_v)):
            acc[...] += lax.dot_general(
                z[level * r :, :], z[level * r : (level + 1) * r, :], (((1,), (1,)), ((), ())),
                preferred_element_type=F32,
            )

    acc_g[...] = jnp.zeros_like(acc_g)
    acc_r[...] = jnp.zeros_like(acc_r)
    acc_v[...] = jnp.zeros_like(acc_v)
    fill(za, 0)

    def step(i, carry):
        fill(zb, 2 * i + 1)
        gram(za)
        fill(za, jnp.minimum(2 * i + 2, chunks - 1))
        gram(zb)
        return carry

    lax.fori_loop(0, chunks // 2, step, 0)
    cross = acc_r[r : 2 * r, :]
    factor = spd_factor(prior_ref[0] + acc_v[:r, :])
    for i in range(3):
        factor_ref[i] = factor[i]
    s = acc_r[:r, :] - mm(cross, spd_apply(factor, cross), 0, 0)
    pair_ref[...] = jnp.concatenate([s[:h, :h], s[:h, h:], s[h:, h:]], axis=1)


def leaf_rest_kernel(half_ref, scale_ref, kg_ref, kr_ref, kl_ref, sites_ref, factor_ref, acc_g, acc_r, acc_v,
                     solved_ref, cross_ref, keep_ref, send_ref, table_ref, pieces):
    r = acc_g.shape[1]
    h = r // 2
    y_cols = jnp.transpose(jnp.concatenate([acc_g[3 * r :, :], acc_r[2 * r :, :], acc_v[r:, :]], axis=1))
    cross_g = acc_g[2 * r : 3 * r, :]
    cross_r = acc_r[r : 2 * r, :]
    factor = (factor_ref[0], factor_ref[1], factor_ref[2])
    x = spd_apply(factor, jnp.concatenate([cross_g, cross_r, y_cols[2 * r :]], axis=1))
    solved_ref[...] = x
    x = jnp.concatenate([x[:, :r], x[:, 2 * r :]], axis=1)
    rows = jnp.concatenate([acc_g[r : 2 * r, :], y_cols[r : 2 * r]], axis=1) - mm(cross_r, x, 0, 0)
    cross_ref[...] = jnp.concatenate([rows[:h, :r], rows[h:, :r], rows[:h, r:], rows[h:, r:]], axis=1)
    upper = jnp.concatenate([acc_g[:r, :], y_cols[:r]], axis=1) - mm(cross_g, x, 0, 0)
    pieces[0], pieces[1] = pack_halves(upper)
    keep_ref[...] = pieces[half_ref[0]]
    send_ref[...] = pieces[1 - half_ref[0]]
    knots = knot_columns((kg_ref, kr_ref, kl_ref))
    for level in range(3):
        table_ref[level * r : (level + 1) * r, :] = basis(
            knots, level, sites_ref[0:1, :], sites_ref[1:2, :], scale_ref[level]
        )


def region_factor_kernel(own_ref, other_ref, prior_ref, after_ref, factor_ref):
    h = own_ref.shape[0]
    s = own_ref[...] + other_ref[...]
    lower = jnp.concatenate([s[:, h : 2 * h], s[:, 2 * h :]], axis=0)
    upper = jnp.concatenate([s[:, :h], jnp.zeros_like(s[:, :h])], axis=0)
    factor = spd_factor(prior_ref[0] + jnp.concatenate([upper, lower], axis=1))
    for i in range(3):
        factor_ref[i] = factor[i]


def region_kernel(half_ref, factor_ref, own_ref, other_ref, solved_ref, keep_ref, send_ref, pieces):
    h = own_ref.shape[0]
    r = 2 * h
    rows = own_ref[...] + other_ref[...]
    fields = (rows.shape[1] - 2 * r) // 2
    cross = jnp.concatenate([rows[:, :r], rows[:, r : 2 * r]], axis=0)
    y = jnp.concatenate([rows[:, 2 * r : 2 * r + fields], rows[:, 2 * r + fields :]], axis=0)
    x = spd_apply((factor_ref[0], factor_ref[1], factor_ref[2]), jnp.concatenate([cross, y], axis=1))
    solved_ref[...] = x
    pieces[0], pieces[1] = pack_halves(-mm(cross, x, 0, 0))
    keep_ref[...] = pieces[half_ref[0]]
    send_ref[...] = pieces[1 - half_ref[0]]


def combine_kernel(region_ref, leaf_ref, table_ref, slope_ref, base_ref):
    r = region_ref.shape[0]
    leaf_table = table_ref[2 * r :, :]
    upper = table_ref[: 2 * r, :] - mm(leaf_ref[:, : 2 * r], leaf_table, 0, 0)
    slope_ref[...] = upper[:r] - mm(region_ref[:, :r], upper[r:], 0, 0)
    base_ref[...] = mm(region_ref[:, r:], upper[r:], 0, 0) + mm(leaf_ref[:, 2 * r :], leaf_table, 0, 0)


def global_kernel(half_ref, mine_ref, other_ref, prior_ref, slope_ref, base_ref, out_ref, pieces):
    h = mine_ref.shape[0]
    q = h // 2
    pieces[half_ref[0]] = mine_ref[...]
    pieces[1 - half_ref[0]] = other_ref[...]
    a = pieces[0]
    b = pieces[1]
    top = jnp.concatenate([a[:, : h + q], b[:, h : h + q]], axis=1)
    low = jnp.concatenate([jnp.zeros_like(b[:, :h]), b[:, :h]], axis=1)
    y = jnp.concatenate([a[:, h + q :], b[:, h + q :]], axis=0)
    w_g = spd_apply(spd_factor(prior_ref[...] + jnp.concatenate([top, low], axis=0)), y)
    out_ref[...] = base_ref[...] + mm(w_g, slope_ref[...], 0, 0)


SMEM = pl.BlockSpec(memory_space=pltpu.SMEM)
VMEM = pl.BlockSpec(memory_space=pltpu.VMEM)
ANY = pl.BlockSpec(memory_space=pl.ANY)


def in_vmem(x):
    return pltpu.with_memory_space_constraint(x, pltpu.VMEM)


def shape(*dims):
    return jax.ShapeDtypeStruct(dims, F32)


def cost(flops, transcendentals):
    return pl.CostEstimate(flops=6 * flops, transcendentals=transcendentals, bytes_accessed=1 << 21)


def swap(x, axis, size, mask):
    return lax.ppermute(x, axis, [(i, i ^ mask) for i in range(size)])


def masks(size, first):
    bits = [b for b in range(first, size.bit_length() - 1)]
    return [(3 << (b - 1)) if b >= 3 else (1 << b) for b in bits]


def swap_halfway(x, axis, size):
    steps = masks(size, 0)
    for mask in steps[:-1]:
        x = x + swap(x, axis, size, mask)
    return x, swap(x, axis, size, steps[-1])


def shards(n_region, n_super, obs_coords, obs_values, obs_precision, site_coords, length_scale,
           global_knots, region_knots, leaf_knots, global_prior, region_prior, leaf_prior):
    r = global_knots.shape[1]
    h = r // 2
    fields, nobs = obs_values.shape
    nsite = site_coords.shape[1]
    width = 512
    knots = (global_knots, region_knots, leaf_knots)
    half = (lax.axis_index("super") & 1).astype(jnp.int32)[None]
    tall = [shape((3 - level) * r + fields, r) for level in range(3)]
    z = pltpu.VMEM((3 * r + fields, width), jnp.bfloat16)
    own, factor, acc_g, acc_r, acc_v = pl.pallas_call(
        functools.partial(leaf_kernel, nobs // width),
        out_shape=(shape(h, 3 * h), shape(3, h, h), *tall),
        in_specs=[SMEM] + [VMEM] * 7,
        out_specs=(VMEM,) * 5,
        scratch_shapes=[z, z, pltpu.VMEM((r, 8), F32)],
        name="leaf",
        cost_estimate=cost(2 * nobs * (3 * r + fields) ** 2, 3 * r * nobs),
    )(length_scale, *knots, obs_coords, obs_values, obs_precision[None, :], leaf_prior)
    own, other = swap_halfway(own, "region", n_region)
    pieces = pltpu.VMEM((2, h, r), F32)
    solved, cross, keep, send, table = pl.pallas_call(
        leaf_rest_kernel,
        out_shape=(shape(r, 2 * r + fields), shape(h, 2 * r + 2 * fields), shape(h, r), shape(h, r), shape(3 * r, nsite)),
        in_specs=[SMEM] * 2 + [VMEM] * 8,
        out_specs=(VMEM,) * 5,
        scratch_shapes=[pieces],
        name="leaf_rest",
        cost_estimate=cost(r * r * (8 * r + 6 * fields), 3 * r * nsite),
    )(half, length_scale, *knots, site_coords, factor, acc_g, acc_r, acc_v)
    region_factor = pl.pallas_call(
        region_factor_kernel,
        out_shape=shape(3, h, h),
        in_specs=[VMEM] * 3 + [ANY],
        out_specs=VMEM,
        name="region_factor",
        cost_estimate=cost(8 * r * r * r, r),
    )(own, in_vmem(other), region_prior, table)
    own, other = swap_halfway(cross, "region", n_region)
    moved = swap(send, "super", n_super, 1)
    upper, upper_moved = swap_halfway(keep + moved, "region", n_region)
    region_solved, keep, send = pl.pallas_call(
        region_kernel,
        out_shape=(shape(r, r + fields), shape(h, r), shape(h, r)),
        in_specs=[SMEM] + [VMEM] * 3,
        out_specs=(VMEM,) * 3,
        scratch_shapes=[pieces],
        name="region",
        cost_estimate=cost(4 * r * r * (r + fields), r),
    )(half, region_factor, own, in_vmem(other))
    mine = keep + upper + upper_moved + swap(send, "super", n_super, 1)
    slope, base = pl.pallas_call(
        combine_kernel,
        out_shape=(shape(r, nsite), shape(fields, nsite)),
        in_specs=[VMEM] * 3,
        out_specs=(VMEM,) * 2,
        name="combine",
        cost_estimate=cost(6 * r * r * nsite, 0),
    )(region_solved, solved, table)
    for mask in masks(n_super, 1):
        moved = swap(mine, "super", n_super, mask)
        mine = mine + moved
    other = swap(mine, "super", n_super, 1)
    return pl.pallas_call(
        global_kernel,
        out_shape=shape(fields, nsite),
        in_specs=[SMEM] + [VMEM] * 5,
        out_specs=VMEM,
        scratch_shapes=[pieces],
        name="predict",
        cost_estimate=cost(8 * r * r * r, r),
    )(half, in_vmem(mine), in_vmem(other), global_prior, slope, base)


def solution(mesh):
    in_specs = (
        P(None, ("region", "super")),
        P(None, ("region", "super")),
        P(("region", "super")),
        P(None, ("region", "super")),
        P(),
        P(),
        P("super", None, None),
        P(("region", "super"), None, None),
        P(),
        P("super", None, None),
        P(("region", "super"), None, None),
    )
    out_specs = P(None, ("region", "super"))
    body = functools.partial(shards, mesh.shape["region"], mesh.shape["super"])

    return jax.shard_map(body, mesh=mesh, in_specs=in_specs, out_specs=out_specs, check_vma=False)
```

```python
import functools

import jax
import jax.numpy as jnp
from jax import lax
from jax.experimental import pallas as pl
from jax.experimental.pallas import tpu as pltpu
from jax.sharding import PartitionSpec as P


HIGH = lax.Precision.HIGHEST
F32 = jnp.float32


def mm(a, b, ca=1, cb=0):
    return lax.dot_general(a, b, (((ca,), (cb,)), ((), ())), precision=HIGH, preferred_element_type=F32)


def spd_inverse(a):
    n = a.shape[0]
    groups = n // 8
    rows = [a[8 * i : 8 * i + 8, :] for i in range(groups)]
    lane = lax.broadcasted_iota(jnp.int32, (8, n), 1)
    sub = lax.broadcasted_iota(jnp.int32, (8, n), 0)

    def col(x, j):
        return jnp.broadcast_to(x[:, j : j + 1], (8, n))

    def row(x, k):
        return jnp.take_along_axis(x, jnp.full((8, n), k, jnp.int32), axis=0, mode="promise_in_bounds")

    for g in range(groups):
        p = rows[g]
        c = [col(p, 8 * g + k) for k in range(8)]
        b = {i: [] for i in range(groups) if i != g}
        for k in range(8):
            for i in b:
                b[i].append(col(rows[i], 8 * g + k))
        inside = (lane >= 8 * g) & (lane < 8 * g + 8)
        p = jnp.where(inside, jnp.where(lane - 8 * g == sub, 1.0, 0.0), p)
        pivot = row(c[0], 0)
        for k in range(8):
            here = sub == k
            r = 1.0 / pivot
            for m in range(k + 1, 8):
                s = row(c[m], k) * r
                left = c[m] - c[k] * s
                if m == k + 1:
                    pivot = row(left, m)
                c[m] = jnp.where(here, s, left)
            s = row(p, k) * r
            p = jnp.where(here, s, p - c[k] * s)
        pr = [row(p, k) for k in range(8)]
        for i in b:
            t = [b[i][k] * pr[k] for k in range(8)]
            while len(t) > 1:
                t = [t[q] + t[q + 1] for q in range(0, len(t), 2)]
            rows[i] = jnp.where(inside, 0.0, rows[i]) - t[0]
        rows[g] = p
    return jnp.concatenate(rows, axis=0)


def spd_factor(a):
    h = a.shape[0] // 2
    a12 = a[:h, h:]
    i1 = spd_inverse(a[:h, :h])
    t = mm(i1, a12)
    i2 = spd_inverse(a[h:, h:] - mm(a12, t, 0, 0))
    return i1, t, i2


def spd_apply(factor, b):
    i1, t, i2 = factor
    h = t.shape[0]
    x2 = mm(i2, b[h:] - mm(t, b[:h], 0, 0))
    x1 = mm(i1, b[:h]) - mm(t, x2)
    return jnp.concatenate([x1, x2], axis=0)


def pack_halves(f):
    h = f.shape[0] // 2
    q = h // 2
    first = jnp.concatenate([f[:h, :h], f[:h, h : h + q], f[:h, 2 * h :]], axis=1)
    second = jnp.concatenate([f[h:, h : 2 * h], f[:h, h + q : 2 * h], f[h:, 2 * h :]], axis=1)
    return first, second


def knot_columns(refs):
    rows = [refs[0][...], refs[1][0], refs[2][0]]
    rows.append(jnp.zeros_like(rows[0]))
    return jnp.transpose(jnp.concatenate(rows, axis=0))


def basis(knots, level, px, py, scale):
    dx = knots[:, 2 * level : 2 * level + 1] - px
    dy = knots[:, 2 * level + 1 : 2 * level + 2] - py
    return jnp.exp((dx * dx + dy * dy) * (-0.5 / (scale * scale)))


def leaf_kernel(chunks, scale_ref, kg_ref, kr_ref, kl_ref, coords_ref, values_ref, prec_ref, prior_ref,
                pair_ref, factor_ref, acc_g, acc_r, acc_v, za, zb, knots_ref):
    r = prior_ref.shape[1]
    h = r // 2
    width = za.shape[1]
    knots_ref[...] = knot_columns((kg_ref, kr_ref, kl_ref))

    def fill(z, chunk):
        cols = pl.ds(pl.multiple_of(chunk * width, width), width)
        px = coords_ref[0:1, cols]
        py = coords_ref[1:2, cols]
        weight = jnp.sqrt(prec_ref[0:1, cols])
        knots = knots_ref[...]
        for level in range(3):
            table = basis(knots, level, px, py, scale_ref[level])
            z[level * r : (level + 1) * r, :] = (table * weight).astype(jnp.bfloat16)
        z[3 * r :, :] = (values_ref[:, cols].astype(F32) * weight).astype(jnp.bfloat16)

    def gram(z):
        for level, acc in enumerate((acc_g, acc_r, acc_v)):
            acc[...] += lax.dot_general(
                z[level * r :, :], z[level * r : (level + 1) * r, :], (((1,), (1,)), ((), ())),
                preferred_element_type=F32,
            )

    acc_g[...] = jnp.zeros_like(acc_g)
    acc_r[...] = jnp.zeros_like(acc_r)
    acc_v[...] = jnp.zeros_like(acc_v)
    fill(za, 0)

    def step(i, carry):
        fill(zb, 2 * i + 1)
        gram(za)
        fill(za, jnp.minimum(2 * i + 2, chunks - 1))
        gram(zb)
        return carry

    lax.fori_loop(0, chunks // 2, step, 0)
    cross = acc_r[r : 2 * r, :]
    factor = spd_factor(prior_ref[0] + acc_v[:r, :])
    for i in range(3):
        factor_ref[i] = factor[i]
    s = acc_r[:r, :] - mm(cross, spd_apply(factor, cross), 0, 0)
    pair_ref[...] = jnp.concatenate([s[:h, :h], s[:h, h:], s[h:, h:]], axis=1)


def leaf_rest_kernel(half_ref, scale_ref, kg_ref, kr_ref, kl_ref, sites_ref, factor_ref, acc_g, acc_r, acc_v,
                     solved_ref, cross_ref, keep_ref, send_ref, table_ref, pieces):
    r = acc_g.shape[1]
    h = r // 2
    y_cols = jnp.transpose(jnp.concatenate([acc_g[3 * r :, :], acc_r[2 * r :, :], acc_v[r:, :]], axis=1))
    cross_g = acc_g[2 * r : 3 * r, :]
    cross_r = acc_r[r : 2 * r, :]
    factor = (factor_ref[0], factor_ref[1], factor_ref[2])
    x = spd_apply(factor, jnp.concatenate([cross_g, cross_r, y_cols[2 * r :]], axis=1))
    solved_ref[...] = x
    x = jnp.concatenate([x[:, :r], x[:, 2 * r :]], axis=1)
    rows = jnp.concatenate([acc_g[r : 2 * r, :], y_cols[r : 2 * r]], axis=1) - mm(cross_r, x, 0, 0)
    cross_ref[...] = jnp.concatenate([rows[:h, :r], rows[h:, :r], rows[:h, r:], rows[h:, r:]], axis=1)
    upper = jnp.concatenate([acc_g[:r, :], y_cols[:r]], axis=1) - mm(cross_g, x, 0, 0)
    pieces[0], pieces[1] = pack_halves(upper)
    keep_ref[...] = pieces[half_ref[0]]
    send_ref[...] = pieces[1 - half_ref[0]]
    knots = knot_columns((kg_ref, kr_ref, kl_ref))
    for level in range(3):
        table_ref[level * r : (level + 1) * r, :] = basis(
            knots, level, sites_ref[0:1, :], sites_ref[1:2, :], scale_ref[level]
        )


def region_factor_kernel(own_ref, other_ref, prior_ref, after_ref, factor_ref):
    h = own_ref.shape[0]
    s = own_ref[...] + other_ref[...]
    lower = jnp.concatenate([s[:, h : 2 * h], s[:, 2 * h :]], axis=0)
    upper = jnp.concatenate([s[:, :h], jnp.zeros_like(s[:, :h])], axis=0)
    factor = spd_factor(prior_ref[0] + jnp.concatenate([upper, lower], axis=1))
    for i in range(3):
        factor_ref[i] = factor[i]


def region_kernel(half_ref, factor_ref, own_ref, other_ref, solved_ref, keep_ref, send_ref, pieces):
    h = own_ref.shape[0]
    r = 2 * h
    rows = own_ref[...] + other_ref[...]
    fields = (rows.shape[1] - 2 * r) // 2
    cross = jnp.concatenate([rows[:, :r], rows[:, r : 2 * r]], axis=0)
    y = jnp.concatenate([rows[:, 2 * r : 2 * r + fields], rows[:, 2 * r + fields :]], axis=0)
    x = spd_apply((factor_ref[0], factor_ref[1], factor_ref[2]), jnp.concatenate([cross, y], axis=1))
    solved_ref[...] = x
    pieces[0], pieces[1] = pack_halves(-mm(cross, x, 0, 0))
    keep_ref[...] = pieces[half_ref[0]]
    send_ref[...] = pieces[1 - half_ref[0]]


def combine_leaf_kernel(leaf_ref, table_ref, upper_ref, base_ref):
    r = leaf_ref.shape[0]
    leaf_table = table_ref[2 * r :, :]
    upper_ref[...] = table_ref[: 2 * r, :] - mm(leaf_ref[:, : 2 * r], leaf_table, 0, 0)
    base_ref[...] = mm(leaf_ref[:, 2 * r :], leaf_table, 0, 0)


def combine_region_kernel(region_ref, upper_ref, leaf_base_ref, slope_ref, base_ref):
    r = region_ref.shape[0]
    region_table = upper_ref[r:, :]
    slope_ref[...] = upper_ref[:r, :] - mm(region_ref[:, :r], region_table, 0, 0)
    base_ref[...] = leaf_base_ref[...] + mm(region_ref[:, r:], region_table, 0, 0)


def global_kernel(half_ref, mine_ref, other_ref, prior_ref, slope_ref, base_ref, out_ref, pieces):
    h = mine_ref.shape[0]
    q = h // 2
    pieces[half_ref[0]] = mine_ref[...]
    pieces[1 - half_ref[0]] = other_ref[...]
    a = pieces[0]
    b = pieces[1]
    top = jnp.concatenate([a[:, : h + q], b[:, h : h + q]], axis=1)
    low = jnp.concatenate([jnp.zeros_like(b[:, :h]), b[:, :h]], axis=1)
    y = jnp.concatenate([a[:, h + q :], b[:, h + q :]], axis=0)
    w_g = spd_apply(spd_factor(prior_ref[...] + jnp.concatenate([top, low], axis=0)), y)
    out_ref[...] = base_ref[...] + mm(w_g, slope_ref[...], 0, 0)


SMEM = pl.BlockSpec(memory_space=pltpu.SMEM)
VMEM = pl.BlockSpec(memory_space=pltpu.VMEM)
ANY = pl.BlockSpec(memory_space=pl.ANY)


def in_vmem(x):
    return pltpu.with_memory_space_constraint(x, pltpu.VMEM)


def shape(*dims):
    return jax.ShapeDtypeStruct(dims, F32)


def cost(flops, transcendentals):
    return pl.CostEstimate(flops=6 * flops, transcendentals=transcendentals, bytes_accessed=1 << 21)


def swap(x, axis, size, mask):
    return lax.ppermute(x, axis, [(i, i ^ mask) for i in range(size)])


def masks(size, first):
    bits = [b for b in range(first, size.bit_length() - 1)]
    return [(3 << (b - 1)) if b >= 3 else (1 << b) for b in bits]


def swap_halfway(x, axis, size):
    steps = masks(size, 0)
    for mask in steps[:-1]:
        x = x + swap(x, axis, size, mask)
    return x, swap(x, axis, size, steps[-1])


def shards(n_region, n_super, obs_coords, obs_values, obs_precision, site_coords, length_scale,
           global_knots, region_knots, leaf_knots, global_prior, region_prior, leaf_prior):
    r = global_knots.shape[1]
    h = r // 2
    fields, nobs = obs_values.shape
    nsite = site_coords.shape[1]
    width = 512
    knots = (global_knots, region_knots, leaf_knots)
    half = (lax.axis_index("super") & 1).astype(jnp.int32)[None]
    tall = [shape((3 - level) * r + fields, r) for level in range(3)]
    z = pltpu.VMEM((3 * r + fields, width), jnp.bfloat16)
    own, factor, acc_g, acc_r, acc_v = pl.pallas_call(
        functools.partial(leaf_kernel, nobs // width),
        out_shape=(shape(h, 3 * h), shape(3, h, h), *tall),
        in_specs=[SMEM] + [VMEM] * 7,
        out_specs=(VMEM,) * 5,
        scratch_shapes=[z, z, pltpu.VMEM((r, 8), F32)],
        name="leaf",
        cost_estimate=cost(2 * nobs * (3 * r + fields) ** 2, 3 * r * nobs),
    )(length_scale, *knots, obs_coords, obs_values, obs_precision[None, :], leaf_prior)
    own, other = swap_halfway(own, "region", n_region)
    pieces = pltpu.VMEM((2, h, r), F32)
    solved, cross, keep, send, table = pl.pallas_call(
        leaf_rest_kernel,
        out_shape=(shape(r, 2 * r + fields), shape(h, 2 * r + 2 * fields), shape(h, r), shape(h, r), shape(3 * r, nsite)),
        in_specs=[SMEM] * 2 + [VMEM] * 8,
        out_specs=(VMEM,) * 5,
        scratch_shapes=[pieces],
        name="leaf_rest",
        cost_estimate=cost(r * r * (8 * r + 6 * fields), 3 * r * nsite),
    )(half, length_scale, *knots, site_coords, factor, acc_g, acc_r, acc_v)
    region_factor = pl.pallas_call(
        region_factor_kernel,
        out_shape=shape(3, h, h),
        in_specs=[VMEM] * 3 + [ANY],
        out_specs=VMEM,
        name="region_factor",
        cost_estimate=cost(8 * r * r * r, r),
    )(own, in_vmem(other), region_prior, table)
    own, other = swap_halfway(cross, "region", n_region)
    moved = swap(send, "super", n_super, 1)
    upper, upper_moved = swap_halfway(keep + moved, "region", n_region)
    region_solved, keep, send = pl.pallas_call(
        region_kernel,
        out_shape=(shape(r, r + fields), shape(h, r), shape(h, r)),
        in_specs=[SMEM] + [VMEM] * 3,
        out_specs=(VMEM,) * 3,
        scratch_shapes=[pieces],
        name="region",
        cost_estimate=cost(4 * r * r * (r + fields), r),
    )(half, region_factor, own, in_vmem(other))
    mine = keep + upper + upper_moved + swap(send, "super", n_super, 1)
    upper_table, leaf_base = pl.pallas_call(
        combine_leaf_kernel,
        out_shape=(shape(2 * r, nsite), shape(fields, nsite)),
        in_specs=[VMEM] * 2,
        out_specs=(VMEM,) * 2,
        name="combine_leaf",
        cost_estimate=cost(4 * r * r * nsite, 0),
    )(solved, table)
    slope, base = pl.pallas_call(
        combine_region_kernel,
        out_shape=(shape(r, nsite), shape(fields, nsite)),
        in_specs=[VMEM] * 3,
        out_specs=(VMEM,) * 2,
        name="combine_region",
        cost_estimate=cost(2 * r * r * nsite, 0),
    )(region_solved, upper_table, leaf_base)
    for mask in masks(n_super, 1):
        moved = swap(mine, "super", n_super, mask)
        mine = mine + moved
    other = swap(mine, "super", n_super, 1)
    return pl.pallas_call(
        global_kernel,
        out_shape=shape(fields, nsite),
        in_specs=[SMEM] + [VMEM] * 5,
        out_specs=VMEM,
        scratch_shapes=[pieces],
        name="predict",
        cost_estimate=cost(8 * r * r * r, r),
    )(half, in_vmem(mine), in_vmem(other), global_prior, slope, base)


def solution(mesh):
    in_specs = (
        P(None, ("region", "super")),
        P(None, ("region", "super")),
        P(("region", "super")),
        P(None, ("region", "super")),
        P(),
        P(),
        P("super", None, None),
        P(("region", "super"), None, None),
        P(),
        P("super", None, None),
        P(("region", "super"), None, None),
    )
    out_specs = P(None, ("region", "super"))
    body = functools.partial(shards, mesh.shape["region"], mesh.shape["super"])

    return jax.shard_map(body, mesh=mesh, in_specs=in_specs, out_specs=out_specs, check_vma=False)
```
